32 devices in a mesh: dp: 2 (over x), tp: 4 (over z), cp: 4 (over y, core).
Axes of the slice: x: 2, y: 2, z: 4, core: 2. Of those that a mesh axis runs over, the one named last changes fastest.
Arguments:
- c_latent: bfloat16 [4096, 512], P(('dp', 'cp')), parts along dimension 0
- k_rope: bfloat16 [4096, 64], P(('dp', 'cp')), parts along dimension 0
- q_heads: bfloat16 [4096, 128, 192], P(('dp', 'cp'), 'tp'), parts along dimension 0
- d_out: bfloat16 [4096, 128, 128], P(('dp', 'cp'), 'tp'), parts along dimension 0
- w_uk: bfloat16 [512, 128, 128], P(None, 'tp')
- w_uv: bfloat16 [512, 128, 128], P(None, 'tp')
Outputs:
- output 1: bfloat16 [4096, 128, 128], P(('dp', 'cp'), 'tp'), parts along dimension 0
- output 2: float32 [4096, 128, 192], P(('dp', 'cp'), 'tp'), parts along dimension 0
- output 3: float32 [4096, 512], P(('dp', 'cp')), parts along dimension 0
- output 4: float32 [4096, 64], P(('dp', 'cp')), parts along dimension 0
- output 5: float32 [1024, 128, 128], P('dp', 'tp'), parts along dimension 0
- output 6: float32 [1024, 128, 128], P('dp', 'tp'), parts along dimension 0
There are 2 independent parts. The reference program is written for one: setup_inputs(seed, part) draws one part's arguments, and reference() takes and returns one part's arrays. A program takes and returns all parts, laid end to end along the dimension named above; an argument that names none is the same for every part.
All inputs are finite; a program needn't handle non-finite values.
Results may differ from the reference program's by a relative error of at most 0.0148993.
Values are sent between devices in bfloat16 or wider.
A program may use at most 1 GiB of HBM per device.

```python
import jax
import jax.numpy as jnp
from jax import lax

TOK_DEV = 512
CP_SIZE = 4
HEADS = 128
KV_RANK = 512
ROPE_DIM = 64
NOPE_DIM = 128
V_DIM = 128

SEQ_LEN = CP_SIZE * TOK_DEV
HALF_LEN = TOK_DEV // 2
N_PIECES = 2 * CP_SIZE
QK_DIM = NOPE_DIM + ROPE_DIM
NEG_BIG = -1.0e30


def setup_inputs(seed: int = 0, part: int = 0) -> dict:
    base_key = jax.random.key(seed)
    part_key = jax.random.fold_in(base_key, part)
    key_c, key_rope, key_q, key_dout = jax.random.split(part_key, 4)
    key_wk, key_wv = jax.random.split(jax.random.key(seed + 7919), 2)
    c_latent = jax.random.normal(key_c, (SEQ_LEN, KV_RANK), jnp.float32)
    k_rope = jax.random.normal(key_rope, (SEQ_LEN, ROPE_DIM), jnp.float32)
    q_heads = 2.0 * jax.random.normal(key_q, (SEQ_LEN, HEADS, QK_DIM), jnp.float32)
    d_out = jax.random.normal(key_dout, (SEQ_LEN, HEADS, V_DIM), jnp.float32)
    w_uk = jax.random.normal(key_wk, (KV_RANK, HEADS, NOPE_DIM), jnp.float32) * KV_RANK ** -0.5
    w_uv = jax.random.normal(key_wv, (KV_RANK, HEADS, V_DIM), jnp.float32) * KV_RANK ** -0.5
    return {
        'c_latent': c_latent.astype(jnp.bfloat16),
        'k_rope': k_rope.astype(jnp.bfloat16),
        'q_heads': q_heads.astype(jnp.bfloat16),
        'd_out': d_out.astype(jnp.bfloat16),
        'w_uk': w_uk.astype(jnp.bfloat16),
        'w_uv': w_uv.astype(jnp.bfloat16),
    }


def row_positions():
    row_ids = jnp.arange(SEQ_LEN)
    shard_idx = row_ids // TOK_DEV
    within = row_ids % TOK_DEV
    piece_idx = jnp.where(within < HALF_LEN, shard_idx, N_PIECES - 1 - shard_idx)
    return piece_idx * HALF_LEN + within % HALF_LEN


def attend(q_all, knope_all, rope_all, v_all):
    positions = row_positions()
    pos_pieces = positions.reshape(N_PIECES, HALF_LEN)
    qk_scale = QK_DIM ** -0.5

    def head_fn(head_args):
        q_head, knope_head, v_head = head_args
        key_rows = jnp.concatenate([knope_head, rope_all], axis=-1)

        def piece_fn(piece_args):
            q_blk, pos_blk = piece_args
            scores = jnp.dot(q_blk, key_rows.T, preferred_element_type=jnp.float32) * qk_scale
            scores = jnp.where(positions[None, :] <= pos_blk[:, None], scores, NEG_BIG)
            weights = jax.nn.softmax(scores, axis=-1)
            return jnp.dot(weights, v_head, preferred_element_type=jnp.float32)

        out_pieces = lax.map(jax.checkpoint(piece_fn), (q_head.reshape(N_PIECES, HALF_LEN, QK_DIM), pos_pieces))
        return out_pieces.reshape(SEQ_LEN, V_DIM)

    heads_out = lax.map(jax.checkpoint(head_fn), (jnp.transpose(q_all, (1, 0, 2)), jnp.transpose(knope_all, (1, 0, 2)), jnp.transpose(v_all, (1, 0, 2))))
    return jnp.transpose(heads_out, (1, 0, 2))


def reference(c_latent, k_rope, q_heads, d_out, w_uk, w_uv):
    c_wide = c_latent.astype(jnp.float32)
    wk_wide = w_uk.astype(jnp.float32)
    wv_wide = w_uv.astype(jnp.float32)
    knope_all = jnp.einsum('sr,rhd->shd', c_wide, wk_wide).astype(jnp.bfloat16).astype(jnp.float32)
    v_all = jnp.einsum('sr,rhd->shd', c_wide, wv_wide).astype(jnp.bfloat16).astype(jnp.float32)
    out_wide, vjp_fn = jax.vjp(attend, q_heads.astype(jnp.float32), knope_all, k_rope.astype(jnp.float32), v_all)
    dq_heads, dk_nope, dk_rope, dv_all = vjp_fn(d_out.astype(jnp.float32))
    dc_latent = jnp.einsum('shd,rhd->sr', dk_nope, wk_wide) + jnp.einsum('shd,rhd->sr', dv_all, wv_wide)
    dw_uk = jnp.einsum('sr,shd->rhd', c_wide, dk_nope)
    dw_uv = jnp.einsum('sr,shd->rhd', c_wide, dv_all)
    return (out_wide.astype(jnp.bfloat16), dq_heads, dc_latent, dk_rope, dw_uk, dw_uv)
```

```python
import functools
import jax
import jax.numpy as jnp
from jax import lax
from jax.experimental import pallas as pl
from jax.experimental.pallas import tpu as pltpu
from jax.sharding import PartitionSpec as P

NEG_BIG = -1.0e30
LOG2E = 1.4426950408889634
F32 = jnp.float32
BF16 = jnp.bfloat16
CHUNKS = (8, 8, 8, 8)
POST = 'mid'


def mm(a, b):
    return jnp.dot(a, b, preferred_element_type=F32)


def mm_nt(a, b):
    return lax.dot_general(a, b, (((1,), (1,)), ((), ())), preferred_element_type=F32)


def attn_body(n_cp, half, scale, first, n_h, *refs):
    n_blk = n_cp
    c_refs, rt_refs = refs[:n_blk], refs[n_blk:2 * n_blk]
    qt_ref, do_ref, wk_ref, wv_ref, wk_old, wv_old = refs[2 * n_blk:2 * n_blk + 6]
    rest = refs[2 * n_blk + 6:]
    if not first:
        keep_in, send_in = rest[0], rest[1]
        rest = rest[4:]
    (ot_ref, dqt_ref, keep_ref, send_ref, dwk_ref, dws_ref,
     ct, kk, kt, v_s, vt_s, p_s, dkv, dr_s, o_s, dq_s, q_s, qt_s, dot_s, bias, dw_s) = rest
    h = pl.program_id(0)
    me = lax.axis_index('cp')
    d_nope = do_ref.shape[2]
    d_qk = qt_ref.shape[1]
    d_rope = d_qk - d_nope
    blk, _ = c_refs[0].shape
    keys = blk * n_blk
    n_t = 2 * n_cp + 1
    c2 = scale * LOG2E
    acc_refs = [(keep_ref, 0), (send_ref, 0), (keep_ref, 1), (send_ref, 1)]
    even = lax.rem(me, 2) == 0

    @pl.when(h == 0)
    def _():
        for j in range(n_blk):
            rows = slice(j * blk, (j + 1) * blk)
            ct[:, rows] = c_refs[j][...].T
            rt = rt_refs[j][...]
            kt[d_nope:, rows] = rt
            kk[rows, d_nope:] = jnp.concatenate([rt, jnp.zeros((128 - d_rope, blk), BF16)], axis=0).T
        qt_s[d_qk:, :] = jnp.zeros((qt_s.shape[0] - d_qk, qt_s.shape[1]), BF16)
        dr_s[...] = jnp.zeros_like(dr_s)
        dkv[...] = jnp.zeros_like(dkv)
        k_io = lax.broadcasted_iota(jnp.int32, (half, half), 0)
        q_io = lax.broadcasted_iota(jnp.int32, (half, half), 1)
        bias[0] = jnp.zeros((half, half), F32)
        bias[1] = jnp.where(k_io <= q_io, 0.0, NEG_BIG)
        if first:
            keep_ref[...] = jnp.zeros_like(keep_ref)
            send_ref[...] = jnp.zeros_like(send_ref)
        else:
            keep_ref[...] = keep_in[...]
            send_ref[...] = send_in[...]

    def post(j, w):
        rows = slice(j * half, (j + 1) * half)
        g = dkv[rows, :].astype(BF16)
        ref, i = acc_refs[j // 2]
        part = mm(ct[:, rows], g)
        dw_s[...] = part if j == 0 else dw_s[...] + part
        o = j % 2 * half
        ref[i, o:o + half, :] += mm_nt(g, w)
        dkv[rows, :] = jnp.zeros((half, dkv.shape[1]), F32)

    def post_out():
        dwk, dwv = dw_s[:, :d_nope], dw_s[:, d_nope:]
        dwk_ref[0] = jnp.where(even, dwk, dwv)
        dws_ref[0] = jnp.where(even, dwv, dwk)

    @pl.when(h < n_h)
    def _():
        w = jnp.concatenate([wk_ref[0], wv_ref[0]], axis=1)
        w_old = jnp.concatenate([wk_old[0], wv_old[0]], axis=1)
        for j in range(0, keys, half):
            rows = slice(j, j + half)
            kv = mm(c_refs[j // blk][j % blk:j % blk + half, :], w).astype(BF16)
            kk[rows, :d_nope] = kv[:, :d_nope]
            v_s[rows, :] = kv[:, d_nope:]
            kt[:d_nope, rows] = kv[:, :d_nope].T
            vt_s[:, rows] = kv[:, d_nope:].T
        qt_s[:d_qk, :] = qt_ref[0]
        q_s[...] = qt_s[...].T
        dot_s[...] = do_ref[0].T

        tiles = []
        for t in range(n_t):
            if t == 0:
                is_a, qo, kp = True, 0, 0
            elif t < n_cp:
                is_a = t <= me
                qo = pl.multiple_of(jnp.where(is_a, 0, half), half)
                kp = jnp.where(is_a, t, t - me - 1)
            else:
                is_a, qo, kp = None, half, t - me - 1
            low = kp < n_cp
            owner = jnp.where(low, kp, 2 * n_cp - 1 - kp)
            ko = pl.multiple_of(jnp.bitwise_xor(owner, me) * blk + jnp.where(low, 0, half), half)
            tiles.append((t, is_a, qo, ko))

        def pick(is_a, a, b):
            return b if is_a is None else a if is_a is True else jnp.where(is_a, a, b)

        def put(is_a, cur, new):
            a, b = cur
            if is_a is True:
                return (new, b)
            if is_a is None:
                return (a, new)
            return (jnp.where(is_a, new, a), jnp.where(is_a, b, new))

        neg = jnp.full((1, half), NEG_BIG, F32)
        zero = jnp.zeros((1, half), F32)
        m, l = (neg, neg), (zero, zero)
        for t, is_a, qo, ko in tiles:
            s = mm(kk[pl.ds(ko, half), :], qt_s[:, pl.ds(qo, half)])
            if t == n_t - 1:
                s = s + bias[1]
            elif t < n_cp:
                s = s + bias[jnp.where(t == me, 1, 0)]
            p_s[t] = s
            m = put(is_a, m, jnp.maximum(pick(is_a, *m), jnp.max(s, axis=0, keepdims=True)))
        m = tuple(x * c2 for x in m)
        acc_o = None
        for t, is_a, qo, ko in tiles:
            p = jnp.exp2(p_s[t] * c2 - pick(is_a, *m))
            l = put(is_a, l, pick(is_a, *l) + jnp.sum(p, axis=0, keepdims=True))
            p_s[t] = p
            o = mm(vt_s[:, pl.ds(ko, half)], p.astype(BF16))
            if t == 0:
                o_s[:, :half] = o
                o_s[:, half:] = jnp.zeros_like(o)
            elif t < n_cp:
                o_s[:, pl.ds(qo, half)] += o
            else:
                acc_o = o if acc_o is None else acc_o + o
            if POST == 'mid' and t < 2 * n_blk:
                post(t, w_old)
        o_s[:, half:] += acc_o
        if POST == 'mid':
            post_out()
        linv = tuple(1.0 / x for x in l)
        dd = []
        for i in range(2):
            cols = slice(i * half, (i + 1) * half)
            o = o_s[:, cols] * linv[i]
            ot_ref[0, :, cols] = o.astype(BF16)
            dd.append(jnp.sum(o * dot_s[:, cols].astype(F32), axis=0, keepdims=True))

        acc_q = None
        for t, is_a, qo, ko in tiles:
            p = p_s[t] * (pick(is_a, *linv))
            rows = pl.ds(ko, half)
            dp = mm(v_s[rows, :], dot_s[:, pl.ds(qo, half)])
            ds = (p * (dp - pick(is_a, *dd))).astype(BF16)
            dv = mm(p.astype(BF16), do_ref[0, pl.ds(qo, half), :])
            dk = mm(ds, q_s[pl.ds(qo, half), :]) * scale
            dq = mm(kt[:, rows], ds)
            dkv[rows, :d_nope] += dk[:, :d_nope]
            dkv[rows, d_nope:] += dv
            dr_s[rows, :] += dk[:, d_nope:]
            if t == 0:
                dq_s[:, :half] = dq
                dq_s[:, half:] = jnp.zeros_like(dq)
            elif t < n_cp:
                dq_s[:, pl.ds(qo, half)] += dq
            else:
                acc_q = dq if acc_q is None else acc_q + dq
        dqt_ref[0, :, :half] = dq_s[:, :half] * scale
        dqt_ref[0, :, half:] = (dq_s[:, half:] + acc_q) * scale

    @pl.when(h == n_h)
    def _():
        w_old = jnp.concatenate([wk_old[0], wv_old[0]], axis=1)
        for j in range(2 * n_blk):
            post(j, w_old)
        for j in range(n_blk):
            ref, i = acc_refs[j]
            ref[i, blk:, :] += dr_s[j * blk:(j + 1) * blk, :].T[:d_rope, :]
        post_out()


def attn_call(n_cp, scale, h0, n_h, cs, rts, qt, do_h, wk_h, wv_h, carry):
    heads, d_qk, rows = qt.shape
    blk, rank = cs[0].shape
    d_rope = rts[0].shape[0]
    keys = blk * n_cp
    d_val = do_h.shape[2]
    half = rows // 2
    n_t = 2 * n_cp + 1
    first = carry is None
    full = lambda *shape: pl.BlockSpec(shape, lambda h: (0,) * len(shape))
    head = lambda *shape: pl.BlockSpec((1,) + shape, lambda h: (jnp.minimum(h, n_h - 1) + h0,) + (0,) * len(shape))
    prev = lambda *shape: pl.BlockSpec((1,) + shape, lambda h: (jnp.maximum(h - 1, 0) + h0,) + (0,) * len(shape))
    local = lambda *shape: pl.BlockSpec((1,) + shape, lambda h: (jnp.maximum(h - 1, 0),) + (0,) * len(shape))
    in_specs = [full(blk, rank)] * n_cp + [full(d_rope, blk)] * n_cp + [
        head(d_qk, rows), head(rows, d_val), head(rank, d_val), head(rank, d_val),
        prev(rank, d_val), prev(rank, d_val)]
    args = [*cs, *rts, qt, do_h, wk_h, wv_h, wk_h, wv_h]
    aliases = {}
    acc = (2, blk + d_rope, rank)
    if not first:
        ot, dqt, keep, send = carry
        n = len(args)
        in_specs += [full(*acc), full(*acc), pl.BlockSpec(memory_space=pl.ANY), pl.BlockSpec(memory_space=pl.ANY)]
        args += [keep, send, ot, dqt]
        aliases = {n + 2: 0, n + 3: 1}
    out_shape = [jax.ShapeDtypeStruct((heads, d_val, rows), BF16),
                 jax.ShapeDtypeStruct((heads, d_qk, rows), F32),
                 jax.ShapeDtypeStruct(acc, F32),
                 jax.ShapeDtypeStruct(acc, F32),
                 jax.ShapeDtypeStruct((n_h, rank, d_val), F32),
                 jax.ShapeDtypeStruct((n_h, rank, d_val), F32)]
    out_specs = [head(d_val, rows), head(d_qk, rows), full(*acc), full(*acc), local(rank, d_val), local(rank, d_val)]
    scratch = [pltpu.VMEM((rank, keys), BF16),
               pltpu.VMEM((keys, 256), BF16), pltpu.VMEM((d_qk, keys), BF16),
               pltpu.VMEM((keys, d_val), BF16), pltpu.VMEM((d_val, keys), BF16),
               pltpu.VMEM((n_t, half, half), F32),
               pltpu.VMEM((keys, 2 * d_val), F32), pltpu.VMEM((keys, 128), F32),
               pltpu.VMEM((d_val, rows), F32), pltpu.VMEM((d_qk, rows), F32),
               pltpu.VMEM((rows, 256), BF16), pltpu.VMEM((256, rows), BF16),
               pltpu.VMEM((d_val, rows), BF16), pltpu.VMEM((2, half, half), F32), pltpu.VMEM((rank, 2 * d_val), F32)]
    flops = n_h * (3 * 2 * keys * rank * 2 * d_val + n_t * half * half * 2 * 1024)
    return pl.pallas_call(
        functools.partial(attn_body, n_cp, half, scale, first, n_h),
        grid=(n_h + 1,), in_specs=in_specs, out_specs=out_specs, out_shape=out_shape,
        scratch_shapes=scratch, input_output_aliases=aliases,
        compiler_params=pltpu.CompilerParams(dimension_semantics=("arbitrary",), vmem_limit_bytes=60 * 2**20),
        cost_estimate=pl.CostEstimate(flops=flops, bytes_accessed=n_h * 2**20, transcendentals=0),
        name="attn",
    )(*args)


def place_body(sizes, *refs):
    n = len(sizes)
    mine, other = refs[:n], refs[n:2 * n]
    k_ref, v_ref = refs[-2:]
    even = lax.rem(lax.axis_index('cp'), 2) == 0
    o = 0
    for i, n_h in enumerate(sizes):
        for j in range(n_h):
            a, b = mine[i][j], other[i][j]
            k_ref[:, o, :] = jnp.where(even, a, b)
            v_ref[:, o, :] = jnp.where(even, b, a)
            o += 1


def place(group, heads, mine, other, carry):
    sizes = [x.shape[0] for x in mine]
    n_g = sum(sizes)
    _, rank, d_val = mine[0].shape
    step = 128
    ins = [pl.BlockSpec((n_h, step, d_val), lambda r: (0, r, 0)) for n_h in sizes] * 2
    args = [*mine, *other]
    aliases = {}
    if carry is not None:
        aliases = {len(args): 0, len(args) + 1: 1}
        args += list(carry)
        ins = ins + [pl.BlockSpec(memory_space=pl.ANY)] * 2
    out = jax.ShapeDtypeStruct((rank, heads, d_val), F32)
    return pl.pallas_call(
        functools.partial(place_body, sizes), grid=(rank // step,), in_specs=ins,
        out_specs=[pl.BlockSpec((step, n_g, d_val), lambda r: (r, group, 0))] * 2,
        out_shape=[out, out], input_output_aliases=aliases,
        compiler_params=pltpu.CompilerParams(dimension_semantics=("arbitrary",)),
        cost_estimate=pl.CostEstimate(flops=10 ** 9, bytes_accessed=4 * n_g * rank * d_val * 4, transcendentals=0),
        name="place",
    )(*args)


def swap(x, axis, size, bit):
    return lax.ppermute(x, axis, [(i, i ^ bit) for i in range(size)])


def solution(mesh):
    n_cp = mesh.shape['cp']
    seq_spec = P(('dp', 'cp'), None)
    head_spec = P(('dp', 'cp'), 'tp', None)
    weight_spec = P(None, 'tp', None)
    grad_spec = P('dp', 'tp', None)

    def device_body(c_latent, k_rope, q_heads, d_out, w_uk, w_uv):
        rows = c_latent.shape[0]
        scale = q_heads.shape[2] ** -0.5
        heads = q_heads.shape[1]
        n_tp = mesh.shape['tp']
        rt = k_rope.T
        c2, r2 = swap(c_latent, 'cp', n_cp, 2), swap(rt, 'cp', n_cp, 2)
        c1, r1 = swap(c_latent, 'cp', n_cp, 1), swap(rt, 'cp', n_cp, 1)
        c3, r3 = swap(c2, 'cp', n_cp, 1), swap(r2, 'cp', n_cp, 1)
        cs, rts = (c_latent, c1, c2, c3), (rt, r1, r2, r3)
        qt = jnp.transpose(q_heads, (1, 2, 0))
        do_h = jnp.transpose(d_out, (1, 0, 2))
        wk_h = jnp.transpose(w_uk, (1, 0, 2))
        wv_h = jnp.transpose(w_uv, (1, 0, 2))
        carry = None
        h0 = 0
        mine, other = [], []
        placed = None
        for n_h in CHUNKS:
            *carry, dw_keep, dw_send = attn_call(n_cp, scale, h0, n_h, cs, rts, qt, do_h, wk_h, wv_h, carry)
            h0 += n_h
            chip = dw_keep + swap(dw_send, 'cp', n_cp, 1)
            far = swap(chip, 'cp', n_cp, 2)
            total = chip + far
            mine.append(total)
            other.append(swap(total, 'cp', n_cp, 1))
            if h0 % 8 == 0:
                placed = place(h0 // 8 - 1, heads, mine, other, placed)
                mine, other = [], []
        ot, dqt, keep, send = carry
        chip = keep + swap(send, 'cp', n_cp, 1)
        acc = chip[0] + swap(chip[1], 'cp', n_cp, 2)
        odd = lax.rem(lax.axis_index('tp'), 2) == 1
        outs = []
        cols = acc.shape[1] // 2
        for i in range(2):
            x = acc[:, i * cols:(i + 1) * cols]
            mid = x.shape[0] // 2
            lo, hi = x[:mid], x[mid:]
            x = jnp.where(odd, hi, lo) + swap(jnp.where(odd, lo, hi), 'tp', n_tp, 1)
            x = x + swap(x, 'tp', n_tp, 2)
            y = swap(x, 'tp', n_tp, 1)
            outs.append(jnp.concatenate([jnp.where(odd, y, x), jnp.where(odd, x, y)], axis=0))
        acc = jnp.concatenate(outs, axis=1)
        return (jnp.transpose(ot, (2, 0, 1)), jnp.transpose(dqt, (2, 0, 1)), acc[:rows], acc[rows:].T, placed[0], placed[1])

    return jax.shard_map(device_body, mesh=mesh,
                         in_specs=(seq_spec, seq_spec, head_spec, head_spec, weight_spec, weight_spec),
                         out_specs=(head_spec, head_spec, seq_spec, seq_spec, grad_spec, grad_spec),
                         check_vma=False)
```

```python
import functools
import jax
import jax.numpy as jnp
from jax import lax
from jax.experimental import pallas as pl
from jax.experimental.pallas import tpu as pltpu
from jax.sharding import PartitionSpec as P

NEG_BIG = -1.0e30
LOG2E = 1.4426950408889634
F32 = jnp.float32
BF16 = jnp.bfloat16
Y_HEADS = 24


def mm(a, b):
    return jnp.dot(a, b, preferred_element_type=F32)


def mm_nt(a, b):
    return lax.dot_general(a, b, (((1,), (1,)), ((), ())), preferred_element_type=F32)


def attn_body(n_cp, half, scale, n_h, n_y, *refs):
    n_blk = n_cp
    c_refs, rt_refs = refs[:n_blk], refs[n_blk:2 * n_blk]
    qt_ref, do_ref, wk_ref, wv_ref, wk_old, wv_old = refs[2 * n_blk:2 * n_blk + 6]
    rest = refs[2 * n_blk + 6:]
    (ot_ref, dqt_ref, acc0, acc1, acc2, acc3, done_ref, part_ref,
     ct, kk, kt, v_s, vt_s, p_s, dkv, dr_s, o_s, dq_s, q_s, qt_s, dot_s, bias, dw_s,
     snd, own, chip, far, d_send, d_recv, y_send, y_recv, out_sem) = rest
    h = pl.program_id(0)
    me = lax.axis_index('cp')
    d_nope = do_ref.shape[2]
    d_qk = qt_ref.shape[1]
    d_rope = d_qk - d_nope
    blk, _ = c_refs[0].shape
    keys = blk * n_blk
    n_t = 2 * n_cp + 1
    c2 = scale * LOG2E
    acc_refs = [acc0, acc1, acc2, acc3]
    even = lax.rem(me, 2) == 0
    mate = me + 1 - 2 * lax.rem(me, 2)
    across = lax.rem(me + 2, n_cp)

    def to_mate(g, slot):
        return pltpu.make_async_remote_copy(
            src_ref=snd.at[slot], dst_ref=chip.at[g], send_sem=d_send.at[slot], recv_sem=d_recv.at[g],
            device_id={'cp': mate}, device_id_type=pl.DeviceIdType.MESH)

    def to_across(g):
        return pltpu.make_async_remote_copy(
            src_ref=chip.at[g], dst_ref=far.at[g], send_sem=y_send.at[g], recv_sem=y_recv.at[g],
            device_id={'cp': across}, device_id_type=pl.DeviceIdType.MESH)

    def to_part(g):
        return pltpu.make_async_copy(chip.at[g], part_ref.at[g - n_y], out_sem.at[g])

    def to_done(g):
        return pltpu.make_async_copy(far.at[g], done_ref.at[g], out_sem.at[g])

    def merge(g, slot):
        to_mate(g, slot).wait()
        chip[g] += own[slot]

        @pl.when(g < n_y)
        def _():
            to_across(g).start()

        @pl.when(g >= n_y)
        def _():
            to_part(g).start()

    @pl.when(h == 0)
    def _():
        barrier = pltpu.get_barrier_semaphore()
        for peer in (mate, across):
            pl.semaphore_signal(barrier, inc=1, device_id={'cp': peer}, device_id_type=pl.DeviceIdType.MESH)
        pl.semaphore_wait(barrier, 2)
        for j in range(n_blk):
            rows = slice(j * blk, (j + 1) * blk)
            ct[:, rows] = c_refs[j][...].T
            rt = rt_refs[j][...]
            kt[d_nope:, rows] = rt
            kk[rows, d_nope:] = jnp.concatenate([rt, jnp.zeros((128 - d_rope, blk), BF16)], axis=0).T
        qt_s[d_qk:, :] = jnp.zeros((qt_s.shape[0] - d_qk, qt_s.shape[1]), BF16)
        dr_s[...] = jnp.zeros_like(dr_s)
        dkv[...] = jnp.zeros_like(dkv)
        k_io = lax.broadcasted_iota(jnp.int32, (half, half), 0)
        q_io = lax.broadcasted_iota(jnp.int32, (half, half), 1)
        bias[0] = jnp.zeros((half, half), F32)
        bias[1] = jnp.where(k_io <= q_io, 0.0, NEG_BIG)
        for ref in acc_refs:
            ref[...] = jnp.zeros_like(ref)

    def post(j, w):
        rows = slice(j * half, (j + 1) * half)
        g = dkv[rows, :].astype(BF16)
        ref = acc_refs[j // 2]
        part = mm(ct[:, rows], g)
        dw_s[...] = part if j == 0 else dw_s[...] + part
        o = j % 2 * half
        ref[o:o + half, :] += mm_nt(g, w)
        dkv[rows, :] = jnp.zeros((half, dkv.shape[1]), F32)

    def post_out():
        slot = lax.rem(h + 1, 2)
        dwk, dwv = dw_s[:, :d_nope], dw_s[:, d_nope:]
        own[slot] = jnp.where(even, dwk, dwv)
        snd[slot] = jnp.where(even, dwv, dwk)

    @pl.when(h < n_h)
    def _():
        w = jnp.concatenate([wk_ref[0], wv_ref[0]], axis=1)
        w_old = jnp.concatenate([wk_old[0], wv_old[0]], axis=1)
        for j in range(0, keys, half):
            rows = slice(j, j + half)
            kv = mm(c_refs[j // blk][j % blk:j % blk + half, :], w).astype(BF16)
            kk[rows, :d_nope] = kv[:, :d_nope]
            v_s[rows, :] = kv[:, d_nope:]
            kt[:d_nope, rows] = kv[:, :d_nope].T
            vt_s[:, rows] = kv[:, d_nope:].T
        qt_s[:d_qk, :] = qt_ref[0]
        q_s[...] = qt_s[...].T
        dot_s[...] = do_ref[0].T

        tiles = []
        for t in range(n_t):
            if t == 0:
                is_a, qo, kp = True, 0, me * 0
            elif t < n_cp:
                is_a = t <= me
                qo = pl.multiple_of(jnp.where(is_a, 0, half), half)
                kp = jnp.where(is_a, t, t - me - 1)
            else:
                is_a, qo, kp = None, half, t - me - 1
            low = kp < n_cp
            owner = jnp.where(low, kp, 2 * n_cp - 1 - kp)
            e0, e1 = lax.rem(owner, 2) + lax.rem(me, 2), lax.div(owner, 2) + lax.div(me, 2)
            slot = lax.rem(e0, 2) + 2 * lax.rem(e1, 2)
            ko = pl.multiple_of(slot * blk + jnp.where(low, 0, half), half)
            tiles.append((t, is_a, qo, ko))

        def pick(is_a, a, b):
            return b if is_a is None else a if is_a is True else jnp.where(is_a, a, b)

        def put(is_a, cur, new):
            a, b = cur
            if is_a is True:
                return (new, b)
            if is_a is None:
                return (a, new)
            return (jnp.where(is_a, new, a), jnp.where(is_a, b, new))

        neg = jnp.full((1, half), NEG_BIG, F32)
        zero = jnp.zeros((1, half), F32)
        m, l = (neg, neg), (zero, zero)
        for t, is_a, qo, ko in tiles:
            s = mm(kk[pl.ds(ko, half), :], qt_s[:, pl.ds(qo, half)])
            if t == n_t - 1:
                s = s + bias[1]
            elif t < n_cp:
                s = s + bias[jnp.where(t == me, 1, 0)]
            p_s[t] = s
            m = put(is_a, m, jnp.maximum(pick(is_a, *m), jnp.max(s, axis=0, keepdims=True)))
        m = tuple(x * c2 for x in m)
        acc_o = None
        for t, is_a, qo, ko in tiles:
            p = jnp.exp2(p_s[t] * c2 - pick(is_a, *m))
            l = put(is_a, l, pick(is_a, *l) + jnp.sum(p, axis=0, keepdims=True))
            p_s[t] = p
            o = mm(vt_s[:, pl.ds(ko, half)], p.astype(BF16))
            if t == 0:
                o_s[:, :half] = o
                o_s[:, half:] = jnp.zeros_like(o)
            elif t < n_cp:
                o_s[:, pl.ds(qo, half)] += o
            else:
                acc_o = o if acc_o is None else acc_o + o
            if t < 2 * n_blk:
                post(t, w_old)
        o_s[:, half:] += acc_o
        post_out()
        linv = tuple(1.0 / x for x in l)
        dd = []
        for i in range(2):
            cols = slice(i * half, (i + 1) * half)
            o = o_s[:, cols] * linv[i]
            ot_ref[0, :, cols] = o.astype(BF16)
            dd.append(jnp.sum(o * dot_s[:, cols].astype(F32), axis=0, keepdims=True))

        acc_q = None
        for t, is_a, qo, ko in tiles:
            p = p_s[t] * (pick(is_a, *linv))
            rows = pl.ds(ko, half)
            dp = mm(v_s[rows, :], dot_s[:, pl.ds(qo, half)])
            ds = (p * (dp - pick(is_a, *dd))).astype(BF16)
            dv = mm(p.astype(BF16), do_ref[0, pl.ds(qo, half), :])
            dk = mm(ds, q_s[pl.ds(qo, half), :]) * scale
            dq = mm(kt[:, rows], ds)
            dkv[rows, :d_nope] += dk[:, :d_nope]
            dkv[rows, d_nope:] += dv
            dr_s[rows, :] += dk[:, d_nope:]
            if t == 0:
                dq_s[:, :half] = dq
                dq_s[:, half:] = jnp.zeros_like(dq)
            elif t < n_cp:
                dq_s[:, pl.ds(qo, half)] += dq
            else:
                acc_q = dq if acc_q is None else acc_q + dq
        dqt_ref[0, :, :half] = dq_s[:, :half]
        dqt_ref[0, :, half:] = dq_s[:, half:] + acc_q

        @pl.when(h >= 2)
        def _():
            merge(h - 2, lax.rem(h, 2))

        @pl.when(h >= 1)
        def _():
            to_mate(h - 1, lax.rem(h + 1, 2)).start()

    @pl.when(h == n_h)
    def _():
        w_old = jnp.concatenate([wk_old[0], wv_old[0]], axis=1)
        for j in range(2 * n_blk):
            post(j, w_old)
        for j in range(n_blk):
            acc_refs[j][blk:, :] = dr_s[j * blk:(j + 1) * blk, :].T[:d_rope, :]
        post_out()
        to_mate(n_h - 1, (n_h - 1) % 2).start()
        merge(n_h - 2, n_h % 2)
        merge(n_h - 1, (n_h - 1) % 2)

        def finish(g, carry):
            to_across(g).wait()
            far[g] += chip[g]
            to_done(g).start()
            return carry

        lax.fori_loop(0, n_y, finish, 0)

        def drain(g, carry):
            to_done(g).wait()
            return carry

        lax.fori_loop(0, n_y, drain, 0)
        for g in range(n_y, n_h):
            to_part(g).wait()


def attn_call(n_cp, scale, n_y, cs, rts, qt, do_h, wk_h, wv_h):
    n_h, d_qk, rows = qt.shape
    blk, rank = cs[0].shape
    d_rope = rts[0].shape[0]
    keys = blk * n_cp
    d_val = do_h.shape[2]
    half = rows // 2
    n_t = 2 * n_cp + 1
    full = lambda *shape: pl.BlockSpec(shape, lambda h: (0,) * len(shape))
    head = lambda *shape: pl.BlockSpec((1,) + shape, lambda h: (jnp.minimum(h, n_h - 1),) + (0,) * len(shape))
    prev = lambda *shape: pl.BlockSpec((1,) + shape, lambda h: (jnp.maximum(h - 1, 0),) + (0,) * len(shape))
    anyspec = pl.BlockSpec(memory_space=pl.ANY)
    in_specs = [full(blk, rank)] * n_cp + [full(d_rope, blk)] * n_cp + [
        head(d_qk, rows), head(rows, d_val), head(rank, d_val), head(rank, d_val),
        prev(rank, d_val), prev(rank, d_val)]
    args = [*cs, *rts, qt, do_h, wk_h, wv_h, wk_h, wv_h]
    acc = (blk + d_rope, rank)
    out_shape = [jax.ShapeDtypeStruct((n_h, d_val, rows), BF16),
                 jax.ShapeDtypeStruct((n_h, d_qk, rows), F32),
                 *[jax.ShapeDtypeStruct(acc, F32)] * n_cp,
                 jax.ShapeDtypeStruct((n_y, rank, d_val), F32),
                 jax.ShapeDtypeStruct((n_h - n_y, rank, d_val), F32)]
    out_specs = [head(d_val, rows), head(d_qk, rows), *[full(*acc)] * n_cp, anyspec, anyspec]
    scratch = [pltpu.VMEM((rank, keys), BF16),
               pltpu.VMEM((keys, 256), BF16), pltpu.VMEM((d_qk, keys), BF16),
               pltpu.VMEM((keys, d_val), BF16), pltpu.VMEM((d_val, keys), BF16),
               pltpu.VMEM((n_t, half, half), F32),
               pltpu.VMEM((keys, 2 * d_val), F32), pltpu.VMEM((keys, 128), F32),
               pltpu.VMEM((d_val, rows), F32), pltpu.VMEM((d_qk, rows), F32),
               pltpu.VMEM((rows, 256), BF16), pltpu.VMEM((256, rows), BF16),
               pltpu.VMEM((d_val, rows), BF16), pltpu.VMEM((2, half, half), F32), pltpu.VMEM((rank, 2 * d_val), F32),
               pltpu.VMEM((2, rank, d_val), F32), pltpu.VMEM((2, rank, d_val), F32),
               pltpu.VMEM((n_h, rank, d_val), F32), pltpu.VMEM((n_y, rank, d_val), F32),
               pltpu.SemaphoreType.DMA((2,)), pltpu.SemaphoreType.DMA((n_h,)),
               pltpu.SemaphoreType.DMA((n_y,)), pltpu.SemaphoreType.DMA((n_y,)),
               pltpu.SemaphoreType.DMA((n_h,))]
    flops = n_h * (3 * 2 * keys * rank * 2 * d_val + n_t * half * half * 2 * 1024)
    return pl.pallas_call(
        functools.partial(attn_body, n_cp, half, scale, n_h, n_y),
        grid=(n_h + 1,), in_specs=in_specs, out_specs=out_specs, out_shape=out_shape,
        scratch_shapes=scratch,
        compiler_params=pltpu.CompilerParams(dimension_semantics=("arbitrary",), vmem_limit_bytes=63 * 2**20,
                                             collective_id=0, has_side_effects=True),
        cost_estimate=pl.CostEstimate(flops=flops, bytes_accessed=n_h * 2**20, transcendentals=0),
        name="attn",
    )(*args)


def place_body(mine, other, *refs):
    k_ref, v_ref = refs[-2:]
    even = lax.rem(lax.axis_index('cp'), 2) == 0
    for j in range(mine.shape[0]):
        a, b = mine[j], other[j]
        k_ref[:, j, :] = jnp.where(even, a, b)
        v_ref[:, j, :] = jnp.where(even, b, a)


def place(group, heads, mine, other, carry):
    n_g = 8
    n_h, rank, d_val = mine.shape
    step = 128
    ins = [pl.BlockSpec((n_g, step, d_val), lambda g, r: (g, r, 0))] * 2
    args = [mine, other]
    aliases = {}
    if carry is not None:
        aliases = {2: 0, 3: 1}
        args += list(carry)
        ins = ins + [pl.BlockSpec(memory_space=pl.ANY)] * 2
    out = jax.ShapeDtypeStruct((rank, heads, d_val), F32)
    return pl.pallas_call(
        place_body, grid=(n_h // n_g, rank // step), in_specs=ins,
        out_specs=[pl.BlockSpec((step, n_g, d_val), lambda g, r: (r, g + group, 0))] * 2,
        out_shape=[out, out], input_output_aliases=aliases,
        compiler_params=pltpu.CompilerParams(dimension_semantics=("arbitrary", "arbitrary")),
        cost_estimate=pl.CostEstimate(flops=n_h * 10 ** 8, bytes_accessed=4 * n_h * rank * d_val * 4, transcendentals=0),
        name="place",
    )(*args)


def rows_body(x_ref, o_ref, s_ref):
    for j in range(x_ref.shape[0]):
        s_ref[:, j, :] = x_ref[j].T.astype(F32)
    o_ref[...] = s_ref[...].astype(BF16)


def to_rows(x):
    n_g = 8
    heads, d_val, rows = x.shape
    return pl.pallas_call(
        rows_body, grid=(heads // n_g,),
        in_specs=[pl.BlockSpec((n_g, d_val, rows), lambda g: (g, 0, 0))],
        out_specs=pl.BlockSpec((rows, n_g, d_val), lambda g: (0, g, 0)),
        out_shape=jax.ShapeDtypeStruct((rows, heads, d_val), BF16),
        scratch_shapes=[pltpu.VMEM((rows, n_g, d_val), F32)],
        compiler_params=pltpu.CompilerParams(dimension_semantics=("arbitrary",)),
        cost_estimate=pl.CostEstimate(flops=10 ** 9, bytes_accessed=4 * heads * d_val * rows, transcendentals=0),
        name="to_rows",
    )(x)


def swap(x, axis, size, bit):
    return lax.ppermute(x, axis, [(i, i ^ bit) for i in range(size)])


def solution(mesh):
    n_cp = mesh.shape['cp']
    seq_spec = P(('dp', 'cp'), None)
    head_spec = P(('dp', 'cp'), 'tp', None)
    weight_spec = P(None, 'tp', None)
    grad_spec = P('dp', 'tp', None)

    def device_body(c_latent, k_rope, q_heads, d_out, w_uk, w_uv):
        rows = c_latent.shape[0]
        scale = q_heads.shape[2] ** -0.5
        heads = q_heads.shape[1]
        n_tp = mesh.shape['tp']
        rt = k_rope.T
        c2, r2 = swap(c_latent, 'cp', n_cp, 2), swap(rt, 'cp', n_cp, 2)
        c1, r1 = swap(c_latent, 'cp', n_cp, 1), swap(rt, 'cp', n_cp, 1)
        qt = jnp.transpose(q_heads, (1, 2, 0))
        do_h = jnp.transpose(d_out, (1, 0, 2))
        wk_h = jnp.transpose(w_uk, (1, 0, 2))
        wv_h = jnp.transpose(w_uv, (1, 0, 2))
        c2, r2, do_h, wk_h, wv_h = lax.optimization_barrier((c2, r2, do_h, wk_h, wv_h))
        c3, r3 = swap(c2, 'cp', n_cp, 1), swap(r2, 'cp', n_cp, 1)
        cs, rts = (c_latent, c1, c2, c3), (rt, r1, r2, r3)
        ot, dqt, a0, a1, a2, a3, done, part = attn_call(n_cp, scale, Y_HEADS, cs, rts, qt, do_h, wk_h, wv_h)
        g2 = swap(a3, 'cp', n_cp, 1)
        g0 = swap(a1, 'cp', n_cp, 1)
        dq = jnp.transpose(dqt * scale, (2, 0, 1))
        out = to_rows(ot)
        other = swap(done, 'cp', n_cp, 1)
        placed = place(0, heads, done, other, None)
        odd = lax.rem(lax.axis_index('tp'), 2) == 1
        n_col = a0.shape[1] // 2
        mid = a0.shape[0] // 2
        col = lambda v, i: v[:, i * n_col:(i + 1) * n_col]
        far = []
        for i in range(2):
            far.append(swap(col(a2, i) + col(g2, i), 'cp', n_cp, 2))

        def first_swap(x):
            lo, hi = x[:mid], x[mid:]
            y = swap(jnp.where(odd, lo, hi), 'tp', n_tp, 1)
            return jnp.where(odd, hi, lo) + y

        def last_swaps(x):
            y = swap(x, 'tp', n_tp, 2)
            x = x + y
            y = swap(x, 'tp', n_tp, 1)
            return jnp.concatenate([jnp.where(odd, y, x), jnp.where(odd, x, y)], axis=0)

        x0 = first_swap(col(a0, 0) + col(g0, 0) + far[0])
        x0, far1 = lax.optimization_barrier((x0, far[1]))
        x1 = first_swap(col(a0, 1) + col(g0, 1) + far1)
        halves = [last_swaps(x0), last_swaps(x1)]
        acc = jnp.concatenate(halves, axis=1)
        far = swap(part, 'cp', n_cp, 2)
        far, acc = lax.optimization_barrier((far, acc))
        total = part + far
        placed = place(Y_HEADS // 8, heads, total, swap(total, 'cp', n_cp, 1), placed)
        return (out, dq, acc[:rows], acc[rows:].T, placed[0], placed[1])

    return jax.shard_map(device_body, mesh=mesh,
                         in_specs=(seq_spec, seq_spec, head_spec, head_spec, weight_spec, weight_spec),
                         out_specs=(head_spec, head_spec, seq_spec, seq_spec, grad_spec, grad_spec),
                         check_vma=False)
```

```python
import functools
import jax
import jax.numpy as jnp
from jax import lax
from jax.experimental import pallas as pl
from jax.experimental.pallas import tpu as pltpu
from jax.sharding import PartitionSpec as P

NEG_BIG = -1.0e30
LOG2E = 1.4426950408889634
F32 = jnp.float32
BF16 = jnp.bfloat16
Y_HEADS = 25


def mm(a, b):
    return jnp.dot(a, b, preferred_element_type=F32)


def mm_nt(a, b):
    return lax.dot_general(a, b, (((1,), (1,)), ((), ())), preferred_element_type=F32)


def attn_body(n_cp, half, scale, n_h, n_y, *refs):
    n_blk = n_cp
    c_refs, rt_refs = refs[:n_blk], refs[n_blk:2 * n_blk]
    qt_ref, do_ref, wk_ref, wv_ref, wk_old, wv_old = refs[2 * n_blk:2 * n_blk + 6]
    rest = refs[2 * n_blk + 6:]
    (ot_ref, dqt_ref, acc0, acc1, acc2, acc3, done_ref, part_ref,
     ct, kk, kt, v_s, vt_s, p_s, dkv, dr_s, o_s, dq_s, q_s, qt_s, dot_s, bias, dw_s,
     snd, own, chip, far, d_send, d_recv, y_send, y_recv, out_sem) = rest
    h = pl.program_id(0)
    me = lax.axis_index('cp')
    d_nope = do_ref.shape[2]
    d_qk = qt_ref.shape[1]
    d_rope = d_qk - d_nope
    blk, _ = c_refs[0].shape
    keys = blk * n_blk
    n_t = 2 * n_cp + 1
    c2 = scale * LOG2E
    acc_refs = [acc0, acc1, acc2, acc3]
    even = lax.rem(me, 2) == 0
    mate = me + 1 - 2 * lax.rem(me, 2)
    across = lax.rem(me + 2, n_cp)

    def to_mate(g, slot):
        return pltpu.make_async_remote_copy(
            src_ref=snd.at[slot], dst_ref=chip.at[g], send_sem=d_send.at[slot], recv_sem=d_recv.at[g],
            device_id={'cp': mate}, device_id_type=pl.DeviceIdType.MESH)

    def to_across(g):
        return pltpu.make_async_remote_copy(
            src_ref=chip.at[g], dst_ref=far.at[g], send_sem=y_send.at[g], recv_sem=y_recv.at[g],
            device_id={'cp': across}, device_id_type=pl.DeviceIdType.MESH)

    def to_part(g):
        return pltpu.make_async_copy(chip.at[g], part_ref.at[g - n_y], out_sem.at[g])

    def to_done(g):
        return pltpu.make_async_copy(far.at[g], done_ref.at[g], out_sem.at[g])

    def merge(g, slot):
        to_mate(g, slot).wait()
        chip[g] += own[slot]

    def pass_on(g):
        @pl.when(g < n_y)
        def _():
            to_across(g).start()

        @pl.when(g >= n_y)
        def _():
            to_part(g).start()

    @pl.when(h == 0)
    def _():
        barrier = pltpu.get_barrier_semaphore()
        for peer in (mate, across):
            pl.semaphore_signal(barrier, inc=1, device_id={'cp': peer}, device_id_type=pl.DeviceIdType.MESH)
        pl.semaphore_wait(barrier, 2)
        for j in range(n_blk):
            rows = slice(j * blk, (j + 1) * blk)
            ct[:, rows] = c_refs[j][...].T
            rt = rt_refs[j][...]
            kt[d_nope:, rows] = rt
            kk[rows, d_nope:] = jnp.concatenate([rt, jnp.zeros((128 - d_rope, blk), BF16)], axis=0).T
        qt_s[d_qk:, :] = jnp.zeros((qt_s.shape[0] - d_qk, qt_s.shape[1]), BF16)
        dr_s[...] = jnp.zeros_like(dr_s)
        dkv[...] = jnp.zeros_like(dkv)
        k_io = lax.broadcasted_iota(jnp.int32, (half, half), 0)
        q_io = lax.broadcasted_iota(jnp.int32, (half, half), 1)
        bias[0] = jnp.zeros((half, half), F32)
        bias[1] = jnp.where(k_io <= q_io, 0.0, NEG_BIG)
        for ref in acc_refs:
            ref[...] = jnp.zeros_like(ref)

    def post(j, w):
        rows = slice(j * half, (j + 1) * half)
        g = dkv[rows, :].astype(BF16)
        ref = acc_refs[j // 2]
        part = mm(ct[:, rows], g)
        dw_s[...] = part if j == 0 else dw_s[...] + part
        o = j % 2 * half
        ref[o:o + half, :] += mm_nt(g, w)
        dkv[rows, :] = jnp.zeros((half, dkv.shape[1]), F32)

    def post_out():
        slot = lax.rem(h + 1, 2)
        dwk, dwv = dw_s[:, :d_nope], dw_s[:, d_nope:]
        own[slot] = jnp.where(even, dwk, dwv)
        snd[slot] = jnp.where(even, dwv, dwk)

    @pl.when(h < n_h)
    def _():
        w = jnp.concatenate([wk_ref[0], wv_ref[0]], axis=1)
        w_old = jnp.concatenate([wk_old[0], wv_old[0]], axis=1)
        for j in range(0, keys, half):
            rows = slice(j, j + half)
            kv = mm(c_refs[j // blk][j % blk:j % blk + half, :], w).astype(BF16)
            kk[rows, :d_nope] = kv[:, :d_nope]
            v_s[rows, :] = kv[:, d_nope:]
            kt[:d_nope, rows] = kv[:, :d_nope].T
            vt_s[:, rows] = kv[:, d_nope:].T
        qt_s[:d_qk, :] = qt_ref[0]
        q_s[...] = qt_s[...].T
        dot_s[...] = do_ref[0].T

        tiles = []
        for t in range(n_t):
            if t == 0:
                is_a, qo, kp = True, 0, me * 0
            elif t < n_cp:
                is_a = t <= me
                qo = pl.multiple_of(jnp.where(is_a, 0, half), half)
                kp = jnp.where(is_a, t, t - me - 1)
            else:
                is_a, qo, kp = None, half, t - me - 1
            low = kp < n_cp
            owner = jnp.where(low, kp, 2 * n_cp - 1 - kp)
            e0, e1 = lax.rem(owner, 2) + lax.rem(me, 2), lax.div(owner, 2) + lax.div(me, 2)
            slot = lax.rem(e0, 2) + 2 * lax.rem(e1, 2)
            ko = pl.multiple_of(slot * blk + jnp.where(low, 0, half), half)
            tiles.append((t, is_a, qo, ko))

        def pick(is_a, a, b):
            return b if is_a is None else a if is_a is True else jnp.where(is_a, a, b)

        def put(is_a, cur, new):
            a, b = cur
            if is_a is True:
                return (new, b)
            if is_a is None:
                return (a, new)
            return (jnp.where(is_a, new, a), jnp.where(is_a, b, new))

        neg = jnp.full((1, half), NEG_BIG, F32)
        zero = jnp.zeros((1, half), F32)
        m, l = (neg, neg), (zero, zero)
        for t, is_a, qo, ko in tiles:
            s = mm(kk[pl.ds(ko, half), :], qt_s[:, pl.ds(qo, half)])
            if t == n_t - 1:
                s = s + bias[1]
            elif t < n_cp:
                s = s + bias[jnp.where(t == me, 1, 0)]
            p_s[t] = s
            m = put(is_a, m, jnp.maximum(pick(is_a, *m), jnp.max(s, axis=0, keepdims=True)))
        m = tuple(x * c2 for x in m)
        acc_o = None
        for t, is_a, qo, ko in tiles:
            p = jnp.exp2(p_s[t] * c2 - pick(is_a, *m))
            l = put(is_a, l, pick(is_a, *l) + jnp.sum(p, axis=0, keepdims=True))
            p_s[t] = p
            o = mm(vt_s[:, pl.ds(ko, half)], p.astype(BF16))
            if t == 0:
                o_s[:, :half] = o
                o_s[:, half:] = jnp.zeros_like(o)
            elif t < n_cp:
                o_s[:, pl.ds(qo, half)] += o
            else:
                acc_o = o if acc_o is None else acc_o + o
            if t < 2 * n_blk:
                post(t, w_old)
        o_s[:, half:] += acc_o
        post_out()
        linv = tuple(1.0 / x for x in l)
        dd = []
        for i in range(2):
            cols = slice(i * half, (i + 1) * half)
            o = o_s[:, cols] * linv[i]
            ot_ref[0, :, cols] = o.astype(BF16)
            dd.append(jnp.sum(o * dot_s[:, cols].astype(F32), axis=0, keepdims=True))

        acc_q = None
        for t, is_a, qo, ko in tiles:
            p = p_s[t] * (pick(is_a, *linv))
            rows = pl.ds(ko, half)
            dp = mm(v_s[rows, :], dot_s[:, pl.ds(qo, half)])
            ds = (p * (dp - pick(is_a, *dd))).astype(BF16)
            dv = mm(p.astype(BF16), do_ref[0, pl.ds(qo, half), :])
            dk = mm(ds, q_s[pl.ds(qo, half), :]) * scale
            dq = mm(kt[:, rows], ds)
            dkv[rows, :d_nope] += dk[:, :d_nope]
            dkv[rows, d_nope:] += dv
            dr_s[rows, :] += dk[:, d_nope:]
            if t == 0:
                dq_s[:, :half] = dq
                dq_s[:, half:] = jnp.zeros_like(dq)
            elif t < n_cp:
                dq_s[:, pl.ds(qo, half)] += dq
            else:
                acc_q = dq if acc_q is None else acc_q + dq
        dqt_ref[0, :, :half] = dq_s[:, :half]
        dqt_ref[0, :, half:] = dq_s[:, half:] + acc_q

        @pl.when(h >= 2)
        def _():
            merge(h - 2, lax.rem(h, 2))

        @pl.when(h >= 1)
        def _():
            to_mate(h - 1, lax.rem(h + 1, 2)).start()

        @pl.when(h >= 2)
        def _():
            pass_on(h - 2)

    @pl.when(h == n_h)
    def _():
        w_old = jnp.concatenate([wk_old[0], wv_old[0]], axis=1)
        for j in range(2 * n_blk):
            post(j, w_old)
        for j in range(n_blk):
            acc_refs[j][blk:, :] = dr_s[j * blk:(j + 1) * blk, :].T[:d_rope, :]
        post_out()
        merge(n_h - 2, n_h % 2)
        to_mate(n_h - 1, (n_h - 1) % 2).start()
        pass_on(n_h - 2)
        merge(n_h - 1, (n_h - 1) % 2)
        pass_on(n_h - 1)

        def finish(g, carry):
            to_across(g).wait()
            far[g] += chip[g]
            to_done(g).start()
            return carry

        lax.fori_loop(0, n_y, finish, 0)

        def drain(g, carry):
            to_done(g).wait()
            return carry

        lax.fori_loop(0, n_y, drain, 0)
        for g in range(n_y, n_h):
            to_part(g).wait()


def attn_call(n_cp, scale, n_y, cs, rts, qt, do_h, wk_h, wv_h):
    n_h, d_qk, rows = qt.shape
    blk, rank = cs[0].shape
    d_rope = rts[0].shape[0]
    keys = blk * n_cp
    d_val = do_h.shape[2]
    half = rows // 2
    n_t = 2 * n_cp + 1
    full = lambda *shape: pl.BlockSpec(shape, lambda h: (0,) * len(shape))
    head = lambda *shape: pl.BlockSpec((1,) + shape, lambda h: (jnp.minimum(h, n_h - 1),) + (0,) * len(shape))
    prev = lambda *shape: pl.BlockSpec((1,) + shape, lambda h: (jnp.maximum(h - 1, 0),) + (0,) * len(shape))
    anyspec = pl.BlockSpec(memory_space=pl.ANY)
    in_specs = [full(blk, rank)] * n_cp + [full(d_rope, blk)] * n_cp + [
        head(d_qk, rows), head(rows, d_val), head(rank, d_val), head(rank, d_val),
        prev(rank, d_val), prev(rank, d_val)]
    args = [*cs, *rts, qt, do_h, wk_h, wv_h, wk_h, wv_h]
    acc = (blk + d_rope, rank)
    out_shape = [jax.ShapeDtypeStruct((n_h, d_val, rows), BF16),
                 jax.ShapeDtypeStruct((n_h, d_qk, rows), F32),
                 *[jax.ShapeDtypeStruct(acc, F32)] * n_cp,
                 jax.ShapeDtypeStruct((n_y, rank, d_val), F32),
                 jax.ShapeDtypeStruct((n_h - n_y, rank, d_val), F32)]
    out_specs = [head(d_val, rows), head(d_qk, rows), *[full(*acc)] * n_cp, anyspec, anyspec]
    scratch = [pltpu.VMEM((rank, keys), BF16),
               pltpu.VMEM((keys, 256), BF16), pltpu.VMEM((d_qk, keys), BF16),
               pltpu.VMEM((keys, d_val), BF16), pltpu.VMEM((d_val, keys), BF16),
               pltpu.VMEM((n_t, half, half), F32),
               pltpu.VMEM((keys, 2 * d_val), F32), pltpu.VMEM((keys, 128), F32),
               pltpu.VMEM((d_val, rows), F32), pltpu.VMEM((d_qk, rows), F32),
               pltpu.VMEM((rows, 256), BF16), pltpu.VMEM((256, rows), BF16),
               pltpu.VMEM((d_val, rows), BF16), pltpu.VMEM((2, half, half), F32), pltpu.VMEM((rank, 2 * d_val), F32),
               pltpu.VMEM((2, rank, d_val), F32), pltpu.VMEM((2, rank, d_val), F32),
               pltpu.VMEM((n_h, rank, d_val), F32), pltpu.VMEM((n_y, rank, d_val), F32),
               pltpu.SemaphoreType.DMA((2,)), pltpu.SemaphoreType.DMA((n_h,)),
               pltpu.SemaphoreType.DMA((n_y,)), pltpu.SemaphoreType.DMA((n_y,)),
               pltpu.SemaphoreType.DMA((n_h,))]
    flops = n_h * (3 * 2 * keys * rank * 2 * d_val + n_t * half * half * 2 * 1024)
    return pl.pallas_call(
        functools.partial(attn_body, n_cp, half, scale, n_h, n_y),
        grid=(n_h + 1,), in_specs=in_specs, out_specs=out_specs, out_shape=out_shape,
        scratch_shapes=scratch,
        compiler_params=pltpu.CompilerParams(dimension_semantics=("arbitrary",), vmem_limit_bytes=63 * 2**20,
                                             collective_id=0, has_side_effects=True),
        cost_estimate=pl.CostEstimate(flops=flops, bytes_accessed=n_h * 2**20, transcendentals=0),
        name="attn",
    )(*args)


def place_body(n_in, *refs):
    mine, other = refs[:n_in], refs[n_in:2 * n_in]
    k_ref, v_ref = refs[-2:]
    even = lax.rem(lax.axis_index('cp'), 2) == 0
    o = 0
    for x, y in zip(mine, other):
        for j in range(x.shape[0]):
            a, b = x[j], y[j]
            k_ref[:, o, :] = jnp.where(even, a, b)
            v_ref[:, o, :] = jnp.where(even, b, a)
            o += 1


def place(group, n_group, heads, parts, carry):
    n_g = 8
    _, rank, d_val = parts[0][0].shape
    step = 128
    ins = [pl.BlockSpec((size, step, d_val), lambda g, r, first=first: (g + first, r, 0)) for _, _, size, first in parts] * 2
    args = [p[0] for p in parts] + [p[1] for p in parts]
    n = len(args)
    aliases = {}
    if carry is not None:
        aliases = {n: 0, n + 1: 1}
        args += list(carry)
        ins = ins + [pl.BlockSpec(memory_space=pl.ANY)] * 2
    out = jax.ShapeDtypeStruct((rank, heads, d_val), F32)
    return pl.pallas_call(
        functools.partial(place_body, len(parts)), grid=(n_group, rank // step), in_specs=ins,
        out_specs=[pl.BlockSpec((step, n_g, d_val), lambda g, r: (r, g + group, 0))] * 2,
        out_shape=[out, out], input_output_aliases=aliases,
        compiler_params=pltpu.CompilerParams(dimension_semantics=("arbitrary", "arbitrary")),
        cost_estimate=pl.CostEstimate(flops=n_group * 10 ** 9, bytes_accessed=4 * n_group * 8 * rank * d_val * 4, transcendentals=0),
        name="place",
    )(*args)


def rows_body(x_ref, o_ref, s_ref):
    for j in range(x_ref.shape[0]):
        s_ref[:, j, :] = x_ref[j].T.astype(F32)
    o_ref[...] = s_ref[...].astype(BF16)


def to_rows(x):
    n_g = 8
    heads, d_val, rows = x.shape
    return pl.pallas_call(
        rows_body, grid=(heads // n_g,),
        in_specs=[pl.BlockSpec((n_g, d_val, rows), lambda g: (g, 0, 0))],
        out_specs=pl.BlockSpec((rows, n_g, d_val), lambda g: (0, g, 0)),
        out_shape=jax.ShapeDtypeStruct((rows, heads, d_val), BF16),
        scratch_shapes=[pltpu.VMEM((rows, n_g, d_val), F32)],
        compiler_params=pltpu.CompilerParams(dimension_semantics=("arbitrary",)),
        cost_estimate=pl.CostEstimate(flops=10 ** 9, bytes_accessed=4 * heads * d_val * rows, transcendentals=0),
        name="to_rows",
    )(x)


def swap(x, axis, size, bit):
    return lax.ppermute(x, axis, [(i, i ^ bit) for i in range(size)])


def solution(mesh):
    n_cp = mesh.shape['cp']
    seq_spec = P(('dp', 'cp'), None)
    head_spec = P(('dp', 'cp'), 'tp', None)
    weight_spec = P(None, 'tp', None)
    grad_spec = P('dp', 'tp', None)

    def device_body(c_latent, k_rope, q_heads, d_out, w_uk, w_uv):
        rows = c_latent.shape[0]
        scale = q_heads.shape[2] ** -0.5
        heads = q_heads.shape[1]
        n_tp = mesh.shape['tp']
        rt = k_rope.T
        c2, r2 = swap(c_latent, 'cp', n_cp, 2), swap(rt, 'cp', n_cp, 2)
        c1, r1 = swap(c_latent, 'cp', n_cp, 1), swap(rt, 'cp', n_cp, 1)
        qt = jnp.transpose(q_heads, (1, 2, 0))
        do_h = jnp.transpose(d_out, (1, 0, 2))
        wk_h = jnp.transpose(w_uk, (1, 0, 2))
        wv_h = jnp.transpose(w_uv, (1, 0, 2))
        c2, r2, do_h, wk_h, wv_h = lax.optimization_barrier((c2, r2, do_h, wk_h, wv_h))
        c3, r3 = swap(c2, 'cp', n_cp, 1), swap(r2, 'cp', n_cp, 1)
        cs, rts = (c_latent, c1, c2, c3), (rt, r1, r2, r3)
        ot, dqt, a0, a1, a2, a3, done, part = attn_call(n_cp, scale, Y_HEADS, cs, rts, qt, do_h, wk_h, wv_h)
        g2 = swap(a3, 'cp', n_cp, 1)
        g0 = swap(a1, 'cp', n_cp, 1)
        dq = jnp.transpose(dqt * scale, (2, 0, 1))
        out = to_rows(ot)
        other = swap(done, 'cp', n_cp, 1)
        whole = Y_HEADS // 8
        placed = place(0, 1, heads, [(done, other, 8, 0)], None)
        placed = place(1, whole - 1, heads, [(done, other, 8, 1)], placed)
        odd = lax.rem(lax.axis_index('tp'), 2) == 1
        n_col = a0.shape[1] // 2
        mid = a0.shape[0] // 2
        col = lambda v, i: v[:, i * n_col:(i + 1) * n_col]
        far = []
        for i in range(2):
            far.append(swap(col(a2, i) + col(g2, i), 'cp', n_cp, 2))

        def first_swap(x):
            lo, hi = x[:mid], x[mid:]
            y = swap(jnp.where(odd, lo, hi), 'tp', n_tp, 1)
            return jnp.where(odd, hi, lo) + y

        def last_swaps(x):
            y = swap(x, 'tp', n_tp, 2)
            x = x + y
            y = swap(x, 'tp', n_tp, 1)
            return jnp.concatenate([jnp.where(odd, y, x), jnp.where(odd, x, y)], axis=0)

        x0 = first_swap(col(a0, 0) + col(g0, 0) + far[0])
        x0, far1 = lax.optimization_barrier((x0, far[1]))
        x1 = first_swap(col(a0, 1) + col(g0, 1) + far1)
        halves = [last_swaps(x0), last_swaps(x1)]
        acc = jnp.concatenate(halves, axis=1)
        far = swap(part, 'cp', n_cp, 2)
        far, acc = lax.optimization_barrier((far, acc))
        total = part + far
        rest = Y_HEADS - whole * 8
        placed = place(whole, 1, heads, [(done, other, rest, Y_HEADS // rest - 1),
                                         (total, swap(total, 'cp', n_cp, 1), heads - Y_HEADS, 0)], placed)
        return (out, dq, acc[:rows], acc[rows:].T, placed[0], placed[1])

    return jax.shard_map(device_body, mesh=mesh,
                         in_specs=(seq_spec, seq_spec, head_spec, head_spec, weight_spec, weight_spec),
                         out_specs=(head_spec, head_spec, seq_spec, seq_spec, grad_spec, grad_spec),
                         check_vma=False)
```
